32 devices in a mesh: grp: 2 (over x), seq: 16 (over z, y, core).
Axes of the slice: x: 2, y: 2, z: 4, core: 2. Of those that a mesh axis runs over, the one named last changes fastest.
Arguments:
- queries: bfloat16 [256, 4096], P(('grp', 'seq')), parts along dimension 0, may hold values from -9 to 9
- question_keys: bfloat16 [256, 2048], P(('grp', 'seq')), parts along dimension 0, may hold values from -4 to 4
- question_values: bfloat16 [256, 2048], P(('grp', 'seq')), parts along dimension 0, may hold values from -5 to 5
- doc_keys: bfloat16 [16384, 2048], P(('grp', 'seq')), parts along dimension 0, may hold values from -4 to 4
- doc_values: bfloat16 [16384, 2048], P(('grp', 'seq')), parts along dimension 0, may hold values from -5 to 5
- lengths: int32 [2], P('grp'), parts along dimension 0, may hold values from 4 to 128
- offsets: int32 [2], P('grp'), parts along dimension 0, may hold values from 2 to 8192, as said below
Outputs:
- attended: bfloat16 [256, 4096], P(('grp', 'seq')), parts along dimension 0
The draws below stay inside these ranges and needn't reach their ends.
There are 2 independent parts, one for each index of `grp`. The reference program is written for one: setup_inputs(seed, part) draws one part's arguments, and reference() takes and returns one part's arrays. A program takes and returns all parts, laid end to end along the dimension named above; each array names one. Nothing has to cross between parts.
Inputs may be any that keep to these rules, and one draw needn't show every extreme that they name: Some question has offsets equal to 8192.
All inputs are finite; a program needn't handle non-finite values.
Results may differ from the reference program's by a relative error of at most 0.0029.
Values may be sent and summed in bfloat16 or wider, within the bound.
A program may use at most 64 MiB of HBM per device.

```python
import jax
import jax.numpy as jnp
from jax import lax

H = 32
KVH = 16
HD = 128
QSCALE = 144
QL = 128
NQ = 1
DOC_DEV = 512
QT = 128
DOC = 8192
N_SEQ = 16


def draw_queries(key, part):
    values = 3.0 * jax.random.normal(jax.random.fold_in(key, 11), (NQ * QL, H * HD), jnp.float32)
    values = jnp.clip(values, -9.0, 9.0)
    return values.astype(jnp.bfloat16)


def draw_doc_keys(key, part):
    values = jax.random.normal(jax.random.fold_in(key, 13), (DOC, KVH * HD), jnp.float32)
    values = jnp.clip(values, -4.0, 4.0)
    return values.astype(jnp.bfloat16)


def draw_offsets(key, part):
    spread = jax.random.randint(jax.random.fold_in(key, 3), (NQ,), 0, DOC - 1)
    shifts = jax.random.randint(jax.random.fold_in(key, 5), (NQ,), 0, 11)
    result = 2 + jnp.right_shift(spread, shifts)
    chosen = jax.random.randint(jax.random.fold_in(key, 9), (), 0, NQ)
    result = jnp.where(jnp.arange(NQ, dtype=jnp.int32) == chosen, DOC, result)
    return result.astype(jnp.int32)


def levels(rng, dims, split, least, top_value):
    def one(dim, parts):
        heights = jax.random.uniform(jax.random.fold_in(jax.random.fold_in(rng, 6), dim), (parts,), jnp.float32, least / len(split), top_value / len(split))
        return jnp.repeat(jnp.exp(heights), dims[dim] // parts).reshape((-1,) + (1,) * (len(dims) - dim - 1))

    loudness = one(*split[0])
    for cut in split[1:]:
        loudness = loudness * one(*cut)
    return loudness


def normal_values(key, dims, width, most, shards=(), held_as=jnp.bfloat16):
    values = width * jax.random.normal(key, dims, jnp.float32)
    if shards:
        values = values * levels(key, dims, shards, -0.22, 0.18)
    return jnp.clip(values, -most, most).astype(held_as)


def setup_inputs(seed: int = 0, part: int = 0) -> dict:
    keys = jax.random.split(jax.random.key(seed), 8)
    part_keys = jax.random.split(jax.random.fold_in(keys[7], part), 8)
    queries = draw_queries(jax.random.fold_in(jax.random.fold_in(keys[7], part), 71), part)
    question_keys = normal_values(part_keys[1], (QT, KVH * HD), 1.0, 4.0, ((0, 16),))
    question_values = normal_values(part_keys[2], (QT, KVH * HD), 1.0, 5.0, ((0, 16),))
    doc_keys = draw_doc_keys(jax.random.fold_in(jax.random.fold_in(keys[7], part), 71), part)
    doc_values = normal_values(part_keys[4], (DOC, KVH * HD), 1.0, 5.0, ((0, 16),))
    lengths = jax.random.randint(part_keys[5], (NQ,), 4, QL + 1).astype(jnp.int32)
    offsets = draw_offsets(jax.random.fold_in(jax.random.fold_in(keys[7], part), 71), part)
    return {"queries": queries, "question_keys": question_keys, "question_values": question_values, "doc_keys": doc_keys, "doc_values": doc_values, "lengths": lengths, "offsets": offsets}


MASKED = -1.0e30


def row_tables(start, count, lengths, offsets):
    rows = start + jnp.arange(count, dtype=jnp.int32)
    question = rows // QL
    position = rows % QL
    owner_table = question[:, None] == jnp.arange(NQ, dtype=jnp.int32)[None, :]
    row_length = jnp.sum(jnp.where(owner_table, lengths[None, :], 0), axis=1)
    row_offset = jnp.sum(jnp.where(owner_table, offsets[None, :], 0), axis=1)
    return question, position, position < row_length, row_offset


def rounded(values):
    narrow = lax.optimization_barrier(values.astype(jnp.bfloat16))
    return narrow.astype(jnp.float32)


def reference(queries, question_keys, question_values, doc_keys, doc_values, lengths, offsets):
    total_rows = NQ * QL
    rows_block = total_rows // N_SEQ
    per_group = H // KVH
    factor_q = QSCALE ** -0.5
    question, position, live_rows, row_offset = row_tables(0, total_rows, lengths, offsets)
    query_all = queries.astype(jnp.float32).reshape(total_rows, KVH, per_group, HD)

    def visit(state, block):
        row_top, numer, denom = state
        doc_start = (block * DOC_DEV).astype(jnp.int32)
        self_start = (block * rows_block).astype(jnp.int32)
        key_doc = lax.dynamic_slice_in_dim(doc_keys, doc_start, DOC_DEV, 0).astype(jnp.float32).reshape(DOC_DEV, KVH, HD)
        value_doc = lax.dynamic_slice_in_dim(doc_values, doc_start, DOC_DEV, 0).astype(jnp.float32).reshape(DOC_DEV, KVH, HD)
        key_self = lax.dynamic_slice_in_dim(question_keys, self_start, rows_block, 0).astype(jnp.float32).reshape(rows_block, KVH, HD)
        value_self = lax.dynamic_slice_in_dim(question_values, self_start, rows_block, 0).astype(jnp.float32).reshape(rows_block, KVH, HD)
        doc_places = doc_start + jnp.arange(DOC_DEV, dtype=jnp.int32)
        self_rows = self_start + jnp.arange(rows_block, dtype=jnp.int32)
        mask_doc = live_rows[:, None] & (doc_places[None, :] < row_offset[:, None])
        mask_self = live_rows[:, None] & (self_rows[None, :] // QL == question[:, None]) & (self_rows[None, :] % QL <= position[:, None])
        mask_doc = mask_doc[:, None, None, :]
        mask_self = mask_self[:, None, None, :]
        scores_doc = jnp.einsum("rgjd,kgd->rgjk", query_all, key_doc) * factor_q
        scores_self = jnp.einsum("rgjd,kgd->rgjk", query_all, key_self) * factor_q
        scores_doc = jnp.where(mask_doc, scores_doc, MASKED)
        scores_self = jnp.where(mask_self, scores_self, MASKED)
        block_top = jnp.maximum(jnp.max(scores_doc, axis=-1), jnp.max(scores_self, axis=-1))
        weights_doc = rounded(jnp.where(mask_doc, jnp.exp(scores_doc - block_top[..., None]), 0.0))
        weights_self = rounded(jnp.where(mask_self, jnp.exp(scores_self - block_top[..., None]), 0.0))
        block_num = jnp.einsum("rgjk,kgd->rgjd", weights_doc, value_doc) + jnp.einsum("rgjk,kgd->rgjd", weights_self, value_self)
        block_den = jnp.sum(weights_doc, axis=-1) + jnp.sum(weights_self, axis=-1)
        new_top = jnp.maximum(row_top, block_top)
        old_factor = jnp.exp(row_top - new_top)
        new_factor = jnp.exp(block_top - new_top)
        numer = numer * old_factor[..., None] + block_num * new_factor[..., None]
        denom = denom * old_factor + block_den * new_factor
        return (new_top, numer, denom), None

    start_state = (jnp.full((total_rows, KVH, per_group), MASKED, jnp.float32),
                   jnp.zeros((total_rows, KVH, per_group, HD), jnp.float32),
                   jnp.zeros((total_rows, KVH, per_group), jnp.float32))
    final_state, unused = lax.scan(visit, start_state, jnp.arange(N_SEQ, dtype=jnp.int32))
    row_top, numer, denom = final_state
    safe_den = jnp.where(live_rows[:, None, None], denom, 1.0)
    result = numer / safe_den[..., None]
    result = jnp.where(live_rows[:, None, None, None], result, 0.0)
    return result.reshape(total_rows, H * HD).astype(jnp.bfloat16)
```

```python
import functools
import math

import jax
import jax.numpy as jnp
from jax import lax
from jax.experimental import pallas as pl
from jax.experimental.pallas import tpu as pltpu
from jax.sharding import PartitionSpec as P

H = 32
KVH = 16
HD = 128
QSCALE = 144
QL = 128
NQ = 1


MASKED = -1e30


def row_tables(start, count, lengths, offsets):
    rows = start + jnp.arange(count, dtype=jnp.int32)
    question = rows // QL
    position = rows % QL
    owner_table = question[:, None] == jnp.arange(NQ, dtype=jnp.int32)[None, :]
    row_length = jnp.sum(jnp.where(owner_table, lengths[None, :], 0), axis=1)
    row_offset = jnp.sum(jnp.where(owner_table, offsets[None, :], 0), axis=1)
    return (question, position, position < row_length, row_offset)


def local(queries, question_keys, question_values, doc_keys, doc_values, lengths, offsets):
    rows_local = queries.shape[0]
    doc_local = doc_keys.shape[0]
    device_count = lax.axis_size("seq")
    device_index = lax.axis_index("seq")
    total_rows = rows_local * device_count
    per_group = H // KVH
    factor_q = QSCALE ** (-0.5)
    key_doc = doc_keys.reshape(doc_local, KVH, HD)
    value_doc = doc_values.reshape(doc_local, KVH, HD)
    key_self = question_keys.reshape(rows_local, KVH, HD)
    value_self = question_values.reshape(rows_local, KVH, HD)
    doc_places = device_index * doc_local + jnp.arange(doc_local, dtype=jnp.int32)
    self_rows = device_index * rows_local + jnp.arange(rows_local, dtype=jnp.int32)
    whole = lax.all_gather(queries, "seq", axis=0, tiled=True)
    block_rows = math.gcd(total_rows, 512)
    block_count = total_rows // block_rows

    def one_block(start):
        piece = whole.reshape(block_rows, KVH, per_group, HD)
        question, position, live_rows, row_offset = row_tables(start, block_rows, lengths, offsets)
        mask_doc = live_rows[:, None] & (doc_places[None, :] < row_offset[:, None])
        mask_self = (
            live_rows[:, None]
            & (self_rows[None, :] // QL == question[:, None])
            & (self_rows[None, :] % QL <= position[:, None])
        )
        mask_doc = mask_doc[:, None, None, :]
        mask_self = mask_self[:, None, None, :]
        scores_doc = (
            jnp.einsum("rgjd,kgd->rgjk", piece, key_doc, preferred_element_type=jnp.float32)
            * factor_q
        )
        scores_self = (
            jnp.einsum("rgjd,kgd->rgjk", piece, key_self, preferred_element_type=jnp.float32)
            * factor_q
        )
        scores_doc = jnp.where(mask_doc, scores_doc, MASKED)
        scores_self = jnp.where(mask_self, scores_self, MASKED)
        block_top = jnp.maximum(jnp.max(scores_doc, axis=-1), jnp.max(scores_self, axis=-1))
        weights_doc = jnp.where(mask_doc, jnp.exp(scores_doc - block_top[..., None]), 0.0).astype(
            jnp.bfloat16
        )
        weights_self = jnp.where(
            mask_self, jnp.exp(scores_self - block_top[..., None]), 0.0
        ).astype(jnp.bfloat16)
        block_den = jnp.sum(weights_doc.astype(jnp.float32), axis=-1) + jnp.sum(
            weights_self.astype(jnp.float32), axis=-1
        )
        block_num = jnp.einsum(
            "rgjk,kgd->rgjd", weights_doc, value_doc, preferred_element_type=jnp.float32
        )
        block_num = block_num + jnp.einsum(
            "rgjk,kgd->rgjd", weights_self, value_self, preferred_element_type=jnp.float32
        )
        return (
            block_num.reshape(block_rows, H * HD),
            block_top.reshape(block_rows, H),
            block_den.reshape(block_rows, H),
        )

    starts = jnp.arange(block_count, dtype=jnp.int32) * block_rows
    numer, row_top, denom = lax.map(one_block, starts)
    numer = numer.reshape(total_rows, H * HD)
    row_top = row_top.reshape(total_rows, H)
    denom = denom.reshape(total_rows, H)
    got_num, got_top, got_den = (
        lax.all_to_all(numer[None], "seq", split_axis=1, concat_axis=0, tiled=True),
        lax.all_to_all(row_top[None], "seq", split_axis=1, concat_axis=0, tiled=True),
        lax.all_to_all(denom[None], "seq", split_axis=1, concat_axis=0, tiled=True),
    )
    overall = jnp.max(got_top, axis=0)
    rescale = jnp.exp(got_top - overall[None])
    total_num = jnp.sum(
        got_num.reshape(device_count, rows_local, H, HD) * rescale[:, :, :, None], axis=0
    )
    total_den = jnp.sum(got_den * rescale, axis=0)
    question, position, live_rows, row_offset = row_tables(
        device_index * rows_local, rows_local, lengths, offsets
    )
    safe_den = jnp.where(live_rows[:, None], total_den, 1.0)
    result = (total_num / safe_den[:, :, None]).reshape(rows_local, H * HD)
    return jnp.where(live_rows[:, None], result, 0.0).astype(jnp.bfloat16)


MESH = pl.DeviceIdType.MESH
LANE = 128
CHUNKS = 4
LOG2E = math.log2(math.e)
WIRE = jnp.int16
WIRE_TOP = 32767.0


def fused_kernel(
    n, q_ref, qk_ref, qv_ref, k_hbm, v_hbm, len_ref, off_ref, o_ref,
    kbuf, vbuf, bias, qbuf, nkeep, skeep, nsend, ssend, narr, sarr, wsend, wstat, warr, wsarr,
    kv_sem, q_send, q_recv, f_send, f_recv, p_send, p_recv, w_send, w_recv,
):
    chips = n // 2
    rows = q_ref.shape[0]
    doc = k_hbm.shape[0]
    keys = kbuf.shape[0]
    half = chips * rows
    total = 2 * half
    group_width = (KVH // CHUNKS) * HD
    wide = (H // CHUNKS) * HD
    heads = H // CHUNKS
    per_group = H // KVH
    me = lax.axis_index("seq")
    chip, core = me // 2, me % 2
    partner = chip * 2 + 1 - core

    def peer(d):
        return lax.rem(chip + d, chips)

    def kv_copies(c):
        cols = pl.ds(c * group_width, group_width)
        return (
            pltpu.make_async_copy(k_hbm.at[:, cols], kbuf.at[pl.ds(0, doc), cols], kv_sem.at[0, c]),
            pltpu.make_async_copy(v_hbm.at[:, cols], vbuf.at[pl.ds(0, doc), cols], kv_sem.at[1, c]),
        )

    for c in range(CHUNKS):
        for copy in kv_copies(c):
            copy.start()
    barrier = pltpu.get_barrier_semaphore()
    for d in range(1, n):
        pl.semaphore_signal(
            barrier, inc=1, device_id={"seq": lax.rem(me + d, n)}, device_id_type=MESH
        )

    for buf, own in ((kbuf, qk_ref), (vbuf, qv_ref)):
        wide_own = own[...].astype(jnp.float32)
        pad = jnp.zeros((keys - doc - rows, own.shape[1]), jnp.float32)
        buf[doc:, :] = jnp.concatenate([wide_own, pad], axis=0).astype(buf.dtype)
    for c in range(CHUNKS):
        qbuf[c, 0, chip] = q_ref[:, c * wide : (c + 1) * wide]
    slot = lax.broadcasted_iota(jnp.int32, (total, keys), 0)
    place = lax.broadcasted_iota(jnp.int32, (total, keys), 1)
    side = slot // half
    inner = slot % half
    row = (2 * (inner // rows) + jnp.where(side == 0, core, 1 - core)) * rows + inner % rows
    question, position = row // QL, row % QL
    row_length = jnp.zeros_like(row)
    row_offset = jnp.zeros_like(row)
    for i in range(NQ):
        row_length = jnp.where(question == i, len_ref[i], row_length)
        row_offset = jnp.where(question == i, off_ref[i], row_offset)
    self_row = me * rows + place - doc
    seen_doc = (place < doc) & (me * doc + place < row_offset)
    seen_self = (
        (place >= doc) & (place < doc + rows)
        & (self_row // QL == question) & (self_row % QL <= position)
    )
    bias[...] = jnp.where((position < row_length) & (seen_doc | seen_self), 0.0, MASKED)
    pl.semaphore_wait(barrier, n - 1)

    def q_copy(c, d):
        return pltpu.make_async_remote_copy(
            q_ref.at[:, pl.ds(c * wide, wide)], qbuf.at[c, 0, chip],
            q_send.at[c, d], q_recv.at[c, d],
            device_id={"seq": peer(d) * 2 + core}, device_id_type=MESH,
        )

    def f_copy(c, d):
        source = q_ref.at[:, pl.ds(c * wide, wide)] if d == 0 else qbuf.at[c, 0, peer(chips - d)]
        return pltpu.make_async_remote_copy(
            source, qbuf.at[c, 1, peer(chips - d)], f_send.at[c, d], f_recv.at[c, d],
            device_id={"seq": partner}, device_id_type=MESH,
        )

    def p_copies(c):
        return tuple(
            pltpu.make_async_remote_copy(
                a.at[c], b.at[c], p_send.at[c, i], p_recv.at[c, i],
                device_id={"seq": partner}, device_id_type=MESH,
            )
            for i, (a, b) in enumerate(((nsend, narr), (ssend, sarr)))
        )

    def w_copies(c, d):
        return tuple(
            pltpu.make_async_remote_copy(
                a.at[c, peer(d)], b.at[c, chip], w_send.at[c, i, d], w_recv.at[c, i, d],
                device_id={"seq": peer(d) * 2 + core}, device_id_type=MESH,
            )
            for i, (a, b) in enumerate(((wsend, warr), (wstat, wsarr)))
        )

    for c in range(CHUNKS):
        f_copy(c, 0).start()
        for d in range(1, chips):
            q_copy(c, d).start()

    factor = QSCALE ** (-0.5) * LOG2E

    def attend(c):
        for g in range(KVH // CHUNKS):
            cols = slice(c * group_width + g * HD, c * group_width + (g + 1) * HD)
            key, value = kbuf[:, cols], vbuf[:, cols]
            pieces = []
            for j in range(per_group):
                h = g * per_group + j
                block = qbuf[c, :, :, :, h * HD : (h + 1) * HD].astype(jnp.float32)
                pieces.append(block.reshape(total, HD).astype(jnp.bfloat16))
            query = jnp.concatenate(pieces, axis=0)
            scores = lax.dot_general(
                query, key, (((1,), (1,)), ((), ())), preferred_element_type=jnp.float32
            )
            for j in range(per_group):
                h = g * per_group + j
                part = scores[j * total : (j + 1) * total] * factor + bias[...]
                top = jnp.max(part, axis=1, keepdims=True)
                weights = jnp.exp2(part - top).astype(jnp.bfloat16)
                den = jnp.sum(weights.astype(jnp.float32), axis=1, keepdims=True)
                num = jnp.dot(weights, value, preferred_element_type=jnp.float32)
                hc = slice(h * HD, (h + 1) * HD)
                nkeep[c, :, hc] = num[:half]
                nsend[c, :, hc] = num[half:]
                for stat, buf in ((top, 0), (den, heads)):
                    skeep[c, :, buf + h : buf + h + 1] = stat[:half]
                    ssend[c, :, buf + h : buf + h + 1] = stat[half:]

    def pair_up(c):
        for copy in p_copies(c):
            copy.wait_recv()
        stat_a, stat_b = skeep[c], sarr[c]
        top_a, top_b = stat_a[:, :heads], stat_b[:, :heads]
        top = jnp.maximum(top_a, top_b)
        fa, fb = jnp.exp2(top_a - top), jnp.exp2(top_b - top)
        den = stat_a[:, heads : 2 * heads] * fa + stat_b[:, heads : 2 * heads] * fb
        for h in range(heads):
            hc = slice(h * HD, (h + 1) * HD)
            num = nkeep[c, :, hc] * fa[:, h : h + 1] + narr[c, :, hc] * fb[:, h : h + 1]
            largest = jnp.maximum(jnp.max(jnp.abs(num), axis=1, keepdims=True), 1e-30)
            wsend[c, :, :, hc] = encode(num / largest).reshape(chips, rows, HD)
            for stat, at in ((top[:, h : h + 1], h), (den[:, h : h + 1], heads + h), (largest, 2 * heads + h)):
                wstat[c, :, :, at : at + 1] = stat.reshape(chips, rows, 1)
        for d in range(1, chips):
            for copy in w_copies(c, d):
                copy.start()
        warr[c, chip] = wsend[c, chip]
        wsarr[c, chip] = wstat[c, chip]

    for c in range(CHUNKS):
        for d in range(1, chips):
            q_copy(c, d).wait_recv()
            f_copy(c, d).start()
        for d in range(chips):
            f_copy(c, d).wait_recv()
        for copy in kv_copies(c):
            copy.wait()
        attend(c)
        for copy in p_copies(c):
            copy.start()
        if c > 0:
            pair_up(c - 1)
    pair_up(CHUNKS - 1)

    mine = me * rows + lax.broadcasted_iota(jnp.int32, (rows, HD), 0)
    live_to = jnp.zeros_like(mine)
    for i in range(NQ):
        live_to = jnp.where(mine // QL == i, len_ref[i], live_to)
    live = mine % QL < live_to
    for c in range(CHUNKS):
        for d in range(1, chips):
            for copy in w_copies(c, d):
                copy.wait_recv()
        tops = [wsarr[c, k][:, :heads] for k in range(chips)]
        overall = functools.reduce(jnp.maximum, tops)
        shrink = [jnp.exp2(t - overall) for t in tops]
        den = sum(wsarr[c, k][:, heads : 2 * heads] * shrink[k] for k in range(chips))
        coefs = [wsarr[c, k][:, 2 * heads : 3 * heads] * shrink[k] / den for k in range(chips)]
        for h in range(heads):
            hc = slice(h * HD, (h + 1) * HD)
            acc = jnp.zeros((rows, HD), jnp.float32)
            for k in range(chips):
                acc = acc + decode(warr[c, k, :, hc]) * coefs[k][:, h : h + 1]
            o_ref[:, c * wide + h * HD : c * wide + (h + 1) * HD] = jnp.where(live, acc, 0.0).astype(
                o_ref.dtype
            )
    for c in range(CHUNKS):
        f_copy(c, 0).wait_send()
        for d in range(1, chips):
            q_copy(c, d).wait_send()
            f_copy(c, d).wait_send()
            for copy in w_copies(c, d):
                copy.wait_send()
        for copy in p_copies(c):
            copy.wait_send()


def encode(x):
    return jnp.round(x * WIRE_TOP).astype(jnp.int32).astype(WIRE)


def decode(x):
    return x.astype(jnp.int32).astype(jnp.float32) * (1.0 / WIRE_TOP)


def fused(n, queries, question_keys, question_values, doc_keys, doc_values, lengths, offsets):
    rows = queries.shape[0]
    doc = doc_keys.shape[0]
    if rows % 8 or n % 2 or n * rows > 256 or doc % LANE or doc > 1024:
        return local(
            queries, question_keys, question_values, doc_keys, doc_values, lengths, offsets
        )
    chips = n // 2
    half = chips * rows
    keys = doc + -(-rows // LANE) * LANE
    wide = H * HD // CHUNKS
    vmem = pl.BlockSpec(memory_space=pltpu.VMEM)
    smem = pl.BlockSpec(memory_space=pltpu.SMEM)
    hbm = pl.BlockSpec(memory_space=pl.ANY)
    f32 = jnp.float32
    dma = pltpu.SemaphoreType.DMA
    return pl.pallas_call(
        functools.partial(fused_kernel, n),
        out_shape=jax.ShapeDtypeStruct(queries.shape, jnp.bfloat16),
        in_specs=[vmem, vmem, vmem, hbm, hbm, smem, smem],
        out_specs=vmem,
        scratch_shapes=[
            pltpu.VMEM((keys, KVH * HD), jnp.bfloat16),
            pltpu.VMEM((keys, KVH * HD), jnp.bfloat16),
            pltpu.VMEM((2 * half, keys), f32),
            pltpu.VMEM((CHUNKS, 2, chips, rows, wide), jnp.bfloat16),
            pltpu.VMEM((CHUNKS, half, wide), f32),
            pltpu.VMEM((CHUNKS, half, LANE), f32),
            pltpu.VMEM((CHUNKS, half, wide), f32),
            pltpu.VMEM((CHUNKS, half, LANE), f32),
            pltpu.VMEM((CHUNKS, half, wide), f32),
            pltpu.VMEM((CHUNKS, half, LANE), f32),
            pltpu.VMEM((CHUNKS, chips, rows, wide), WIRE),
            pltpu.VMEM((CHUNKS, chips, rows, LANE), f32),
            pltpu.VMEM((CHUNKS, chips, rows, wide), WIRE),
            pltpu.VMEM((CHUNKS, chips, rows, LANE), f32),
            dma((2, CHUNKS)),
            dma((CHUNKS, chips)),
            dma((CHUNKS, chips)),
            dma((CHUNKS, chips)),
            dma((CHUNKS, chips)),
            dma((CHUNKS, 2)),
            dma((CHUNKS, 2)),
            dma((CHUNKS, 2, chips)),
            dma((CHUNKS, 2, chips)),
        ],
        compiler_params=pltpu.CompilerParams(
            collective_id=0, has_side_effects=True, vmem_limit_bytes=60 * 1024 * 1024
        ),
    )(queries, question_keys, question_values, doc_keys, doc_values, lengths, offsets)


def solution(mesh):
    placed = (
        P(("grp", "seq"), None),
        P(("grp", "seq"), None),
        P(("grp", "seq"), None),
        P(("grp", "seq"), None),
        P(("grp", "seq"), None),
        P("grp"),
        P("grp"),
    )
    return jax.shard_map(
        functools.partial(fused, mesh.shape["seq"]),
        mesh=mesh, in_specs=placed, out_specs=P(("grp", "seq"), None), check_vma=False,
    )
```

```python
import functools
import math

import jax
import jax.numpy as jnp
from jax import lax
from jax.experimental import pallas as pl
from jax.experimental.pallas import tpu as pltpu
from jax.sharding import PartitionSpec as P

H = 32
KVH = 16
HD = 128
QSCALE = 144
QL = 128
NQ = 1


MASKED = -1e30


def row_tables(start, count, lengths, offsets):
    rows = start + jnp.arange(count, dtype=jnp.int32)
    question = rows // QL
    position = rows % QL
    owner_table = question[:, None] == jnp.arange(NQ, dtype=jnp.int32)[None, :]
    row_length = jnp.sum(jnp.where(owner_table, lengths[None, :], 0), axis=1)
    row_offset = jnp.sum(jnp.where(owner_table, offsets[None, :], 0), axis=1)
    return (question, position, position < row_length, row_offset)


def local(queries, question_keys, question_values, doc_keys, doc_values, lengths, offsets):
    rows_local = queries.shape[0]
    doc_local = doc_keys.shape[0]
    device_count = lax.axis_size("seq")
    device_index = lax.axis_index("seq")
    total_rows = rows_local * device_count
    per_group = H // KVH
    factor_q = QSCALE ** (-0.5)
    key_doc = doc_keys.reshape(doc_local, KVH, HD)
    value_doc = doc_values.reshape(doc_local, KVH, HD)
    key_self = question_keys.reshape(rows_local, KVH, HD)
    value_self = question_values.reshape(rows_local, KVH, HD)
    doc_places = device_index * doc_local + jnp.arange(doc_local, dtype=jnp.int32)
    self_rows = device_index * rows_local + jnp.arange(rows_local, dtype=jnp.int32)
    whole = lax.all_gather(queries, "seq", axis=0, tiled=True)
    block_rows = math.gcd(total_rows, 512)
    block_count = total_rows // block_rows

    def one_block(start):
        piece = whole.reshape(block_rows, KVH, per_group, HD)
        question, position, live_rows, row_offset = row_tables(start, block_rows, lengths, offsets)
        mask_doc = live_rows[:, None] & (doc_places[None, :] < row_offset[:, None])
        mask_self = (
            live_rows[:, None]
            & (self_rows[None, :] // QL == question[:, None])
            & (self_rows[None, :] % QL <= position[:, None])
        )
        mask_doc = mask_doc[:, None, None, :]
        mask_self = mask_self[:, None, None, :]
        scores_doc = (
            jnp.einsum("rgjd,kgd->rgjk", piece, key_doc, preferred_element_type=jnp.float32)
            * factor_q
        )
        scores_self = (
            jnp.einsum("rgjd,kgd->rgjk", piece, key_self, preferred_element_type=jnp.float32)
            * factor_q
        )
        scores_doc = jnp.where(mask_doc, scores_doc, MASKED)
        scores_self = jnp.where(mask_self, scores_self, MASKED)
        block_top = jnp.maximum(jnp.max(scores_doc, axis=-1), jnp.max(scores_self, axis=-1))
        weights_doc = jnp.where(mask_doc, jnp.exp(scores_doc - block_top[..., None]), 0.0).astype(
            jnp.bfloat16
        )
        weights_self = jnp.where(
            mask_self, jnp.exp(scores_self - block_top[..., None]), 0.0
        ).astype(jnp.bfloat16)
        block_den = jnp.sum(weights_doc.astype(jnp.float32), axis=-1) + jnp.sum(
            weights_self.astype(jnp.float32), axis=-1
        )
        block_num = jnp.einsum(
            "rgjk,kgd->rgjd", weights_doc, value_doc, preferred_element_type=jnp.float32
        )
        block_num = block_num + jnp.einsum(
            "rgjk,kgd->rgjd", weights_self, value_self, preferred_element_type=jnp.float32
        )
        return (
            block_num.reshape(block_rows, H * HD),
            block_top.reshape(block_rows, H),
            block_den.reshape(block_rows, H),
        )

    starts = jnp.arange(block_count, dtype=jnp.int32) * block_rows
    numer, row_top, denom = lax.map(one_block, starts)
    numer = numer.reshape(total_rows, H * HD)
    row_top = row_top.reshape(total_rows, H)
    denom = denom.reshape(total_rows, H)
    got_num, got_top, got_den = (
        lax.all_to_all(numer[None], "seq", split_axis=1, concat_axis=0, tiled=True),
        lax.all_to_all(row_top[None], "seq", split_axis=1, concat_axis=0, tiled=True),
        lax.all_to_all(denom[None], "seq", split_axis=1, concat_axis=0, tiled=True),
    )
    overall = jnp.max(got_top, axis=0)
    rescale = jnp.exp(got_top - overall[None])
    total_num = jnp.sum(
        got_num.reshape(device_count, rows_local, H, HD) * rescale[:, :, :, None], axis=0
    )
    total_den = jnp.sum(got_den * rescale, axis=0)
    question, position, live_rows, row_offset = row_tables(
        device_index * rows_local, rows_local, lengths, offsets
    )
    safe_den = jnp.where(live_rows[:, None], total_den, 1.0)
    result = (total_num / safe_den[:, :, None]).reshape(rows_local, H * HD)
    return jnp.where(live_rows[:, None], result, 0.0).astype(jnp.bfloat16)


MESH = pl.DeviceIdType.MESH
LANE = 128
CHUNKS = 4
LOG2E = math.log2(math.e)
WIRE = jnp.int16
WIRE_TOP = 32767.0


def fused_kernel(
    n, q_ref, qk_ref, qv_ref, k_hbm, v_hbm, len_ref, off_ref, o_ref,
    kbuf, vbuf, bias, qbuf, nkeep, skeep, nsend, ssend, narr, sarr, wsend, wstat, warr, wsarr,
    kv_sem, q_send, q_recv, t_send, t_recv, f_send, f_recv, p_send, p_recv, w_send, w_recv,
):
    chips = n // 2
    rows = q_ref.shape[0]
    doc = k_hbm.shape[0]
    keys = kbuf.shape[0]
    half = chips * rows
    total = 2 * half
    group_width = (KVH // CHUNKS) * HD
    wide = (H // CHUNKS) * HD
    heads = H // CHUNKS
    per_group = H // KVH
    me = lax.axis_index("seq")
    chip, core = me // 2, me % 2
    partner = chip * 2 + 1 - core

    def peer(d):
        return lax.rem(chip + d, chips)

    def kv_copies(c):
        cols = pl.ds(c * group_width, group_width)
        return (
            pltpu.make_async_copy(k_hbm.at[:, cols], kbuf.at[pl.ds(0, doc), cols], kv_sem.at[0, c]),
            pltpu.make_async_copy(v_hbm.at[:, cols], vbuf.at[pl.ds(0, doc), cols], kv_sem.at[1, c]),
        )

    for c in range(CHUNKS):
        for copy in kv_copies(c):
            copy.start()
    barrier = pltpu.get_barrier_semaphore()
    for d in range(1, n):
        pl.semaphore_signal(
            barrier, inc=1, device_id={"seq": lax.rem(me + d, n)}, device_id_type=MESH
        )

    for buf, own in ((kbuf, qk_ref), (vbuf, qv_ref)):
        wide_own = own[...].astype(jnp.float32)
        pad = jnp.zeros((keys - doc - rows, own.shape[1]), jnp.float32)
        buf[doc:, :] = jnp.concatenate([wide_own, pad], axis=0).astype(buf.dtype)
    for c in range(CHUNKS):
        qbuf[c, 0, chip] = q_ref[:, c * wide : (c + 1) * wide]
    slot = lax.broadcasted_iota(jnp.int32, (total, 1), 0)
    place = lax.broadcasted_iota(jnp.int32, (1, keys), 1)
    side = slot // half
    inner = slot % half
    row = (2 * (inner // rows) + jnp.where(side == 0, core, 1 - core)) * rows + inner % rows
    question, position = row // QL, row % QL
    row_length = jnp.zeros_like(row)
    row_offset = jnp.zeros_like(row)
    for i in range(NQ):
        row_length = jnp.where(question == i, len_ref[i], row_length)
        row_offset = jnp.where(question == i, off_ref[i], row_offset)
    doc_end = jnp.where(position < row_length, row_offset - me * doc, 0)
    self_end = jnp.where(position < row_length, row + 1 - me * rows + doc, 0)
    self_start = question * QL - me * rows + doc
    wide_place = jnp.broadcast_to(place, (total, keys))
    seen_doc = (wide_place < doc) & (wide_place < doc_end)
    seen_self = (
        (wide_place >= doc) & (wide_place < doc + rows)
        & (wide_place >= self_start) & (wide_place < self_end)
    )
    bias[...] = jnp.where(seen_doc | seen_self, 0.0, MASKED)
    pl.semaphore_wait(barrier, n - 1)

    lines = chips // 2
    line, col = chip // 2, chip % 2

    def source_chip(e, d):
        return lax.rem(line + lines - d, lines) * 2 + (col if e == 0 else 1 - col)

    def held(c, e, d):
        own = e == 0 and d == 0
        return q_ref.at[:, pl.ds(c * wide, wide)] if own else qbuf.at[c, 0, source_chip(e, d)]

    def q_copy(c, d):
        target = lax.rem(line + d, lines) * 2 + col
        return pltpu.make_async_remote_copy(
            held(c, 0, 0), qbuf.at[c, 0, chip], q_send.at[c, d], q_recv.at[c, d],
            device_id={"seq": target * 2 + core}, device_id_type=MESH,
        )

    def t_copy(c, d):
        return pltpu.make_async_remote_copy(
            held(c, 0, d), qbuf.at[c, 0, source_chip(0, d)], t_send.at[c, d], t_recv.at[c, d],
            device_id={"seq": (line * 2 + 1 - col) * 2 + core}, device_id_type=MESH,
        )

    def f_copy(c, e, d):
        return pltpu.make_async_remote_copy(
            held(c, e, d), qbuf.at[c, 1, source_chip(e, d)],
            f_send.at[c, e, d], f_recv.at[c, e, d],
            device_id={"seq": partner}, device_id_type=MESH,
        )

    def p_copies(c):
        return tuple(
            pltpu.make_async_remote_copy(
                a.at[c], b.at[c], p_send.at[c, i], p_recv.at[c, i],
                device_id={"seq": partner}, device_id_type=MESH,
            )
            for i, (a, b) in enumerate(((nsend, narr), (ssend, sarr)))
        )

    def w_copies(c, d):
        return tuple(
            pltpu.make_async_remote_copy(
                a.at[c, peer(d)], b.at[c, chip], w_send.at[c, i, d], w_recv.at[c, i, d],
                device_id={"seq": peer(d) * 2 + core}, device_id_type=MESH,
            )
            for i, (a, b) in enumerate(((wsend, warr), (wstat, wsarr)))
        )

    for c in range(CHUNKS):
        for d in range(1, lines):
            q_copy(c, d).start()
        t_copy(c, 0).start()
        f_copy(c, 0, 0).start()

    factor = QSCALE ** (-0.5) * LOG2E

    def attend(c):
        for g in range(KVH // CHUNKS):
            cols = slice(c * group_width + g * HD, c * group_width + (g + 1) * HD)
            key, value = kbuf[:, cols], vbuf[:, cols]
            pieces = []
            for j in range(per_group):
                h = g * per_group + j
                block = qbuf[c, :, :, :, h * HD : (h + 1) * HD].astype(jnp.float32)
                pieces.append(block.reshape(total, HD).astype(jnp.bfloat16))
            query = jnp.concatenate(pieces, axis=0)
            scores = lax.dot_general(
                query, key, (((1,), (1,)), ((), ())), preferred_element_type=jnp.float32
            )
            for j in range(per_group):
                h = g * per_group + j
                part = scores[j * total : (j + 1) * total] * factor + bias[...]
                top = jnp.max(part, axis=1, keepdims=True)
                weights = jnp.exp2(part - top).astype(jnp.bfloat16)
                den = jnp.sum(weights.astype(jnp.float32), axis=1, keepdims=True)
                num = jnp.dot(weights, value, preferred_element_type=jnp.float32)
                hc = slice(h * HD, (h + 1) * HD)
                nkeep[c, :, hc] = num[:half]
                largest = row_scale(num)
                nsend[c, :, hc] = encode(num[half:] * (WIRE_TOP / largest[half:]))
                for stat, buf in ((top, 0), (den, heads), (largest, 2 * heads)):
                    skeep[c, :, buf + h : buf + h + 1] = stat[:half]
                    ssend[c, :, buf + h : buf + h + 1] = stat[half:]

    def pair_up(c):
        for copy in p_copies(c):
            copy.wait_recv()
        stat_a, stat_b = skeep[c], sarr[c]
        top_a, top_b = stat_a[:, :heads], stat_b[:, :heads]
        top = jnp.maximum(top_a, top_b)
        fa, fb = jnp.exp2(top_a - top), jnp.exp2(top_b - top)
        fc = fb * stat_b[:, 2 * heads : 3 * heads]
        den = stat_a[:, heads : 2 * heads] * fa + stat_b[:, heads : 2 * heads] * fb
        for h in range(heads):
            hc = slice(h * HD, (h + 1) * HD)
            num = nkeep[c, :, hc] * fa[:, h : h + 1] + decode(narr[c, :, hc]) * fc[:, h : h + 1]
            largest = row_scale(num)
            wsend[c, :, :, hc] = encode(num * (WIRE_TOP / largest)).reshape(chips, rows, HD)
            for stat, at in ((top[:, h : h + 1], h), (den[:, h : h + 1], heads + h), (largest, 2 * heads + h)):
                wstat[c, :, :, at : at + 1] = stat.reshape(chips, rows, 1)
        for d in range(1, chips):
            for copy in w_copies(c, d):
                copy.start()
        warr[c, chip] = wsend[c, chip]
        wsarr[c, chip] = wstat[c, chip]

    def relay_line(c):
        if c < CHUNKS:
            for d in range(1, lines):
                q_copy(c, d).wait_recv()
                t_copy(c, d).start()
                f_copy(c, 0, d).start()

    def relay_twin(c):
        if c < CHUNKS:
            for d in range(lines):
                t_copy(c, d).wait_recv()
                f_copy(c, 1, d).start()

    relay_line(0)
    relay_line(1)
    relay_twin(0)
    for c in range(CHUNKS):
        relay_line(c + 2)
        relay_twin(c + 1)
        for e in range(2):
            for d in range(lines):
                f_copy(c, e, d).wait_recv()
        for copy in kv_copies(c):
            copy.wait()
        attend(c)
        for copy in p_copies(c):
            copy.start()
        if c > 0:
            pair_up(c - 1)
    pair_up(CHUNKS - 1)

    mine = me * rows + lax.broadcasted_iota(jnp.int32, (rows, HD), 0)
    live_to = jnp.zeros_like(mine)
    for i in range(NQ):
        live_to = jnp.where(mine // QL == i, len_ref[i], live_to)
    live = mine % QL < live_to
    for c in range(CHUNKS):
        for d in range(1, chips):
            for copy in w_copies(c, d):
                copy.wait_recv()
        tops = [wsarr[c, k][:, :heads] for k in range(chips)]
        overall = functools.reduce(jnp.maximum, tops)
        shrink = [jnp.exp2(t - overall) for t in tops]
        den = sum(wsarr[c, k][:, heads : 2 * heads] * shrink[k] for k in range(chips))
        coefs = [wsarr[c, k][:, 2 * heads : 3 * heads] * shrink[k] / den for k in range(chips)]
        for h in range(heads):
            hc = slice(h * HD, (h + 1) * HD)
            acc = jnp.zeros((rows, HD), jnp.float32)
            for k in range(chips):
                acc = acc + decode(warr[c, k, :, hc]) * coefs[k][:, h : h + 1]
            o_ref[:, c * wide + h * HD : c * wide + (h + 1) * HD] = jnp.where(live, acc, 0.0).astype(
                o_ref.dtype
            )
    for c in range(CHUNKS):
        for d in range(1, lines):
            q_copy(c, d).wait_send()
        for d in range(lines):
            t_copy(c, d).wait_send()
            for e in range(2):
                f_copy(c, e, d).wait_send()
        for d in range(1, chips):
            for copy in w_copies(c, d):
                copy.wait_send()
        for copy in p_copies(c):
            copy.wait_send()


def row_scale(x):
    return jnp.maximum(jnp.max(jnp.abs(x), axis=1, keepdims=True), 1e-30)


def encode(x):
    return jnp.round(x).astype(jnp.int32).astype(WIRE)


def decode(x):
    return x.astype(jnp.int32).astype(jnp.float32) * (1.0 / WIRE_TOP)


def fused(n, queries, question_keys, question_values, doc_keys, doc_values, lengths, offsets):
    rows = queries.shape[0]
    doc = doc_keys.shape[0]
    if rows % 8 or n % 4 or n * rows > 256 or doc % LANE or doc > 1024:
        return local(
            queries, question_keys, question_values, doc_keys, doc_values, lengths, offsets
        )
    chips = n // 2
    half = chips * rows
    keys = doc + -(-rows // LANE) * LANE
    wide = H * HD // CHUNKS
    vmem = pl.BlockSpec(memory_space=pltpu.VMEM)
    smem = pl.BlockSpec(memory_space=pltpu.SMEM)
    hbm = pl.BlockSpec(memory_space=pl.ANY)
    f32 = jnp.float32
    dma = pltpu.SemaphoreType.DMA
    return pl.pallas_call(
        functools.partial(fused_kernel, n),
        out_shape=jax.ShapeDtypeStruct(queries.shape, jnp.bfloat16),
        in_specs=[vmem, vmem, vmem, hbm, hbm, smem, smem],
        out_specs=vmem,
        scratch_shapes=[
            pltpu.VMEM((keys, KVH * HD), jnp.bfloat16),
            pltpu.VMEM((keys, KVH * HD), jnp.bfloat16),
            pltpu.VMEM((2 * half, keys), f32),
            pltpu.VMEM((CHUNKS, 2, chips, rows, wide), jnp.bfloat16),
            pltpu.VMEM((CHUNKS, half, wide), f32),
            pltpu.VMEM((CHUNKS, half, LANE), f32),
            pltpu.VMEM((CHUNKS, half, wide), WIRE),
            pltpu.VMEM((CHUNKS, half, LANE), f32),
            pltpu.VMEM((CHUNKS, half, wide), WIRE),
            pltpu.VMEM((CHUNKS, half, LANE), f32),
            pltpu.VMEM((CHUNKS, chips, rows, wide), WIRE),
            pltpu.VMEM((CHUNKS, chips, rows, LANE), f32),
            pltpu.VMEM((CHUNKS, chips, rows, wide), WIRE),
            pltpu.VMEM((CHUNKS, chips, rows, LANE), f32),
            dma((2, CHUNKS)),
            dma((CHUNKS, chips // 2)),
            dma((CHUNKS, chips // 2)),
            dma((CHUNKS, chips // 2)),
            dma((CHUNKS, chips // 2)),
            dma((CHUNKS, 2, chips // 2)),
            dma((CHUNKS, 2, chips // 2)),
            dma((CHUNKS, 2)),
            dma((CHUNKS, 2)),
            dma((CHUNKS, 2, chips)),
            dma((CHUNKS, 2, chips)),
        ],
        compiler_params=pltpu.CompilerParams(
            collective_id=0, has_side_effects=True, vmem_limit_bytes=60 * 1024 * 1024
        ),
    )(queries, question_keys, question_values, doc_keys, doc_values, lengths, offsets)


def solution(mesh):
    placed = (
        P(("grp", "seq"), None),
        P(("grp", "seq"), None),
        P(("grp", "seq"), None),
        P(("grp", "seq"), None),
        P(("grp", "seq"), None),
        P("grp"),
        P("grp"),
    )
    return jax.shard_map(
        functools.partial(fused, mesh.shape["seq"]),
        mesh=mesh, in_specs=placed, out_specs=P(("grp", "seq"), None), check_vma=False,
    )
```

```python
import functools
import math

import jax
import jax.numpy as jnp
from jax import lax
from jax.experimental import pallas as pl
from jax.experimental.pallas import tpu as pltpu
from jax.sharding import PartitionSpec as P

H = 32
KVH = 16
HD = 128
QSCALE = 144
QL = 128
NQ = 1


MASKED = -1e30


def row_tables(start, count, lengths, offsets):
    rows = start + jnp.arange(count, dtype=jnp.int32)
    question = rows // QL
    position = rows % QL
    owner_table = question[:, None] == jnp.arange(NQ, dtype=jnp.int32)[None, :]
    row_length = jnp.sum(jnp.where(owner_table, lengths[None, :], 0), axis=1)
    row_offset = jnp.sum(jnp.where(owner_table, offsets[None, :], 0), axis=1)
    return (question, position, position < row_length, row_offset)


def local(queries, question_keys, question_values, doc_keys, doc_values, lengths, offsets):
    rows_local = queries.shape[0]
    doc_local = doc_keys.shape[0]
    device_count = lax.axis_size("seq")
    device_index = lax.axis_index("seq")
    total_rows = rows_local * device_count
    per_group = H // KVH
    factor_q = QSCALE ** (-0.5)
    key_doc = doc_keys.reshape(doc_local, KVH, HD)
    value_doc = doc_values.reshape(doc_local, KVH, HD)
    key_self = question_keys.reshape(rows_local, KVH, HD)
    value_self = question_values.reshape(rows_local, KVH, HD)
    doc_places = device_index * doc_local + jnp.arange(doc_local, dtype=jnp.int32)
    self_rows = device_index * rows_local + jnp.arange(rows_local, dtype=jnp.int32)
    whole = lax.all_gather(queries, "seq", axis=0, tiled=True)
    block_rows = math.gcd(total_rows, 512)
    block_count = total_rows // block_rows

    def one_block(start):
        piece = whole.reshape(block_rows, KVH, per_group, HD)
        question, position, live_rows, row_offset = row_tables(start, block_rows, lengths, offsets)
        mask_doc = live_rows[:, None] & (doc_places[None, :] < row_offset[:, None])
        mask_self = (
            live_rows[:, None]
            & (self_rows[None, :] // QL == question[:, None])
            & (self_rows[None, :] % QL <= position[:, None])
        )
        mask_doc = mask_doc[:, None, None, :]
        mask_self = mask_self[:, None, None, :]
        scores_doc = (
            jnp.einsum("rgjd,kgd->rgjk", piece, key_doc, preferred_element_type=jnp.float32)
            * factor_q
        )
        scores_self = (
            jnp.einsum("rgjd,kgd->rgjk", piece, key_self, preferred_element_type=jnp.float32)
            * factor_q
        )
        scores_doc = jnp.where(mask_doc, scores_doc, MASKED)
        scores_self = jnp.where(mask_self, scores_self, MASKED)
        block_top = jnp.maximum(jnp.max(scores_doc, axis=-1), jnp.max(scores_self, axis=-1))
        weights_doc = jnp.where(mask_doc, jnp.exp(scores_doc - block_top[..., None]), 0.0).astype(
            jnp.bfloat16
        )
        weights_self = jnp.where(
            mask_self, jnp.exp(scores_self - block_top[..., None]), 0.0
        ).astype(jnp.bfloat16)
        block_den = jnp.sum(weights_doc.astype(jnp.float32), axis=-1) + jnp.sum(
            weights_self.astype(jnp.float32), axis=-1
        )
        block_num = jnp.einsum(
            "rgjk,kgd->rgjd", weights_doc, value_doc, preferred_element_type=jnp.float32
        )
        block_num = block_num + jnp.einsum(
            "rgjk,kgd->rgjd", weights_self, value_self, preferred_element_type=jnp.float32
        )
        return (
            block_num.reshape(block_rows, H * HD),
            block_top.reshape(block_rows, H),
            block_den.reshape(block_rows, H),
        )

    starts = jnp.arange(block_count, dtype=jnp.int32) * block_rows
    numer, row_top, denom = lax.map(one_block, starts)
    numer = numer.reshape(total_rows, H * HD)
    row_top = row_top.reshape(total_rows, H)
    denom = denom.reshape(total_rows, H)
    got_num, got_top, got_den = (
        lax.all_to_all(numer[None], "seq", split_axis=1, concat_axis=0, tiled=True),
        lax.all_to_all(row_top[None], "seq", split_axis=1, concat_axis=0, tiled=True),
        lax.all_to_all(denom[None], "seq", split_axis=1, concat_axis=0, tiled=True),
    )
    overall = jnp.max(got_top, axis=0)
    rescale = jnp.exp(got_top - overall[None])
    total_num = jnp.sum(
        got_num.reshape(device_count, rows_local, H, HD) * rescale[:, :, :, None], axis=0
    )
    total_den = jnp.sum(got_den * rescale, axis=0)
    question, position, live_rows, row_offset = row_tables(
        device_index * rows_local, rows_local, lengths, offsets
    )
    safe_den = jnp.where(live_rows[:, None], total_den, 1.0)
    result = (total_num / safe_den[:, :, None]).reshape(rows_local, H * HD)
    return jnp.where(live_rows[:, None], result, 0.0).astype(jnp.bfloat16)


MESH = pl.DeviceIdType.MESH
LANE = 128
CHUNKS = 4
LOG2E = math.log2(math.e)
WIRE = jnp.int16
WIRE_TOP = 32767.0


def fused_kernel(
    n, q_ref, qk_ref, qv_ref, k_hbm, v_hbm, len_ref, off_ref, o_ref,
    kbuf, vbuf, bias, qbuf, nkeep, skeep, nsend, ssend, narr, sarr, wsend, wstat, warr, wsarr,
    kv_sem, q_send, q_recv, f_send, f_recv, p_send, p_recv, w_send, w_recv,
):
    chips = n // 2
    rows = q_ref.shape[0]
    doc = k_hbm.shape[0]
    keys = kbuf.shape[0]
    half = chips * rows
    total = 2 * half
    group_width = (KVH // CHUNKS) * HD
    wide = (H // CHUNKS) * HD
    heads = H // CHUNKS
    per_group = H // KVH
    me = lax.axis_index("seq")
    chip, core = me // 2, me % 2
    partner = chip * 2 + 1 - core

    def peer(d):
        return lax.rem(chip + d, chips)

    def kv_copies(c):
        cols = pl.ds(c * group_width, group_width)
        return (
            pltpu.make_async_copy(k_hbm.at[:, cols], kbuf.at[pl.ds(0, doc), cols], kv_sem.at[0, c]),
            pltpu.make_async_copy(v_hbm.at[:, cols], vbuf.at[pl.ds(0, doc), cols], kv_sem.at[1, c]),
        )

    for c in range(CHUNKS):
        for copy in kv_copies(c):
            copy.start()
    barrier = pltpu.get_barrier_semaphore()
    for d in range(1, n):
        pl.semaphore_signal(
            barrier, inc=1, device_id={"seq": lax.rem(me + d, n)}, device_id_type=MESH
        )

    for buf, own in ((kbuf, qk_ref), (vbuf, qv_ref)):
        wide_own = own[...].astype(jnp.float32)
        pad = jnp.zeros((keys - doc - rows, own.shape[1]), jnp.float32)
        buf[doc:, :] = jnp.concatenate([wide_own, pad], axis=0).astype(buf.dtype)
    for c in range(CHUNKS):
        qbuf[c, 0, chip] = q_ref[:, c * wide : (c + 1) * wide]
    slot = lax.broadcasted_iota(jnp.int32, (total, keys), 0)
    place = lax.broadcasted_iota(jnp.int32, (total, keys), 1)
    side = slot // half
    inner = slot % half
    row = (2 * (inner // rows) + jnp.where(side == 0, core, 1 - core)) * rows + inner % rows
    question, position = row // QL, row % QL
    row_length = jnp.zeros_like(row)
    row_offset = jnp.zeros_like(row)
    for i in range(NQ):
        row_length = jnp.where(question == i, len_ref[i], row_length)
        row_offset = jnp.where(question == i, off_ref[i], row_offset)
    self_row = me * rows + place - doc
    seen_doc = (place < doc) & (me * doc + place < row_offset)
    seen_self = (
        (place >= doc) & (place < doc + rows)
        & (self_row // QL == question) & (self_row % QL <= position)
    )
    bias[...] = jnp.where((position < row_length) & (seen_doc | seen_self), 0.0, MASKED)
    pl.semaphore_wait(barrier, n - 1)

    def q_copy(c, d):
        return pltpu.make_async_remote_copy(
            q_ref.at[:, pl.ds(c * wide, wide)], qbuf.at[c, 0, chip],
            q_send.at[c, d], q_recv.at[c, d],
            device_id={"seq": peer(d) * 2 + core}, device_id_type=MESH,
        )

    def f_copy(c, d):
        source = q_ref.at[:, pl.ds(c * wide, wide)] if d == 0 else qbuf.at[c, 0, peer(chips - d)]
        return pltpu.make_async_remote_copy(
            source, qbuf.at[c, 1, peer(chips - d)], f_send.at[c, d], f_recv.at[c, d],
            device_id={"seq": partner}, device_id_type=MESH,
        )

    def p_copies(c):
        return tuple(
            pltpu.make_async_remote_copy(
                a.at[c], b.at[c], p_send.at[c, i], p_recv.at[c, i],
                device_id={"seq": partner}, device_id_type=MESH,
            )
            for i, (a, b) in enumerate(((nsend, narr), (ssend, sarr)))
        )

    def w_copy(c, d):
        return pltpu.make_async_remote_copy(
            wsend.at[c, peer(d)], warr.at[c, chip], w_send.at[c, d], w_recv.at[c, d],
            device_id={"seq": peer(d) * 2 + core}, device_id_type=MESH,
        )

    def s_copy(d):
        return pltpu.make_async_remote_copy(
            wstat.at[peer(d)], wsarr.at[chip], w_send.at[CHUNKS, d], w_recv.at[CHUNKS, d],
            device_id={"seq": peer(d) * 2 + core}, device_id_type=MESH,
        )

    for c in range(CHUNKS):
        f_copy(c, 0).start()
        for d in range(1, chips):
            q_copy(c, d).start()

    factor = QSCALE ** (-0.5) * LOG2E

    def attend(c):
        for g in range(KVH // CHUNKS):
            cols = slice(c * group_width + g * HD, c * group_width + (g + 1) * HD)
            key, value = kbuf[:, cols], vbuf[:, cols]
            pieces = []
            for j in range(per_group):
                h = g * per_group + j
                block = qbuf[c, :, :, :, h * HD : (h + 1) * HD].astype(jnp.float32)
                pieces.append(block.reshape(total, HD).astype(jnp.bfloat16))
            query = jnp.concatenate(pieces, axis=0)
            scores = lax.dot_general(
                query, key, (((1,), (1,)), ((), ())), preferred_element_type=jnp.float32
            )
            for j in range(per_group):
                h = g * per_group + j
                part = scores[j * total : (j + 1) * total] * factor + bias[...]
                top = jnp.max(part, axis=1, keepdims=True)
                weights = jnp.exp2(part - top).astype(jnp.bfloat16)
                den = jnp.sum(weights.astype(jnp.float32), axis=1, keepdims=True)
                num = jnp.dot(weights, value, preferred_element_type=jnp.float32)
                hc = slice(h * HD, (h + 1) * HD)
                nkeep[c, :, hc] = num[:half]
                nsend[c, :, hc] = num[half:]
                for stat, buf in ((top, 0), (den, heads)):
                    skeep[c, :, buf + h : buf + h + 1] = stat[:half]
                    ssend[c, :, buf + h : buf + h + 1] = stat[half:]

    def pair_up(c):
        for copy in p_copies(c):
            copy.wait_recv()
        stat_a, stat_b = skeep[c], sarr[c]
        top_a, top_b = stat_a[:, :heads], stat_b[:, :heads]
        top = jnp.maximum(top_a, top_b)
        fa, fb = jnp.exp2(top_a - top), jnp.exp2(top_b - top)
        den = stat_a[:, heads : 2 * heads] * fa + stat_b[:, heads : 2 * heads] * fb
        for h in range(heads):
            hc = slice(h * HD, (h + 1) * HD)
            num = nkeep[c, :, hc] * fa[:, h : h + 1] + narr[c, :, hc] * fb[:, h : h + 1]
            largest = jnp.maximum(jnp.max(jnp.abs(num), axis=1, keepdims=True), 1e-30)
            wsend[c, :, :, hc] = encode(num / largest).reshape(chips, rows, HD)
            for kind, stat in enumerate((top[:, h : h + 1], den[:, h : h + 1], largest)):
                at = (c * 3 + kind) * heads + h
                wstat[:, :, at : at + 1] = stat.reshape(chips, rows, 1)
        for d in range(1, chips):
            if c == CHUNKS - 1:
                s_copy(d).start()
            w_copy(c, d).start()
        warr[c, chip] = wsend[c, chip]
        if c == CHUNKS - 1:
            wsarr[chip] = wstat[chip]

    for c in range(CHUNKS):
        for d in range(1, chips):
            q_copy(c, d).wait_recv()
            f_copy(c, d).start()
        for d in range(chips):
            f_copy(c, d).wait_recv()
        for copy in kv_copies(c):
            copy.wait()
        attend(c)
        for copy in p_copies(c):
            copy.start()
        if c > 0:
            pair_up(c - 1)
    pair_up(CHUNKS - 1)

    mine = me * rows + lax.broadcasted_iota(jnp.int32, (rows, HD), 0)
    live_to = jnp.zeros_like(mine)
    for i in range(NQ):
        live_to = jnp.where(mine // QL == i, len_ref[i], live_to)
    live = mine % QL < live_to
    for d in range(1, chips):
        s_copy(d).wait_recv()
    for c in range(CHUNKS):
        for d in range(1, chips):
            w_copy(c, d).wait_recv()
        top_at, den_at, scale_at = ((c * 3 + kind) * heads for kind in range(3))
        tops = [wsarr[k][:, top_at : top_at + heads] for k in range(chips)]
        overall = functools.reduce(jnp.maximum, tops)
        shrink = [jnp.exp2(t - overall) for t in tops]
        den = sum(wsarr[k][:, den_at : den_at + heads] * shrink[k] for k in range(chips))
        coefs = [wsarr[k][:, scale_at : scale_at + heads] * shrink[k] / den for k in range(chips)]
        for h in range(heads):
            hc = slice(h * HD, (h + 1) * HD)
            acc = jnp.zeros((rows, HD), jnp.float32)
            for k in range(chips):
                acc = acc + decode(warr[c, k, :, hc]) * coefs[k][:, h : h + 1]
            o_ref[:, c * wide + h * HD : c * wide + (h + 1) * HD] = jnp.where(live, acc, 0.0).astype(
                o_ref.dtype
            )
    for c in range(CHUNKS):
        f_copy(c, 0).wait_send()
        for d in range(1, chips):
            q_copy(c, d).wait_send()
            f_copy(c, d).wait_send()
            w_copy(c, d).wait_send()
        for copy in p_copies(c):
            copy.wait_send()
    for d in range(1, chips):
        s_copy(d).wait_send()


def encode(x):
    return jnp.round(x * WIRE_TOP).astype(jnp.int32).astype(WIRE)


def decode(x):
    return x.astype(jnp.int32).astype(jnp.float32) * (1.0 / WIRE_TOP)


def fused(n, queries, question_keys, question_values, doc_keys, doc_values, lengths, offsets):
    rows = queries.shape[0]
    doc = doc_keys.shape[0]
    if rows % 8 or n % 2 or n * rows > 256 or doc % LANE or doc > 1024 or 3 * H > LANE:
        return local(
            queries, question_keys, question_values, doc_keys, doc_values, lengths, offsets
        )
    chips = n // 2
    half = chips * rows
    keys = doc + -(-rows // LANE) * LANE
    wide = H * HD // CHUNKS
    vmem = pl.BlockSpec(memory_space=pltpu.VMEM)
    smem = pl.BlockSpec(memory_space=pltpu.SMEM)
    hbm = pl.BlockSpec(memory_space=pl.ANY)
    f32 = jnp.float32
    dma = pltpu.SemaphoreType.DMA
    return pl.pallas_call(
        functools.partial(fused_kernel, n),
        out_shape=jax.ShapeDtypeStruct(queries.shape, jnp.bfloat16),
        in_specs=[vmem, vmem, vmem, hbm, hbm, smem, smem],
        out_specs=vmem,
        scratch_shapes=[
            pltpu.VMEM((keys, KVH * HD), jnp.bfloat16),
            pltpu.VMEM((keys, KVH * HD), jnp.bfloat16),
            pltpu.VMEM((2 * half, keys), f32),
            pltpu.VMEM((CHUNKS, 2, chips, rows, wide), jnp.bfloat16),
            pltpu.VMEM((CHUNKS, half, wide), f32),
            pltpu.VMEM((CHUNKS, half, LANE), f32),
            pltpu.VMEM((CHUNKS, half, wide), f32),
            pltpu.VMEM((CHUNKS, half, LANE), f32),
            pltpu.VMEM((CHUNKS, half, wide), f32),
            pltpu.VMEM((CHUNKS, half, LANE), f32),
            pltpu.VMEM((CHUNKS, chips, rows, wide), WIRE),
            pltpu.VMEM((chips, rows, LANE), f32),
            pltpu.VMEM((CHUNKS, chips, rows, wide), WIRE),
            pltpu.VMEM((chips, rows, LANE), f32),
            dma((2, CHUNKS)),
            dma((CHUNKS, chips)),
            dma((CHUNKS, chips)),
            dma((CHUNKS, chips)),
            dma((CHUNKS, chips)),
            dma((CHUNKS, 2)),
            dma((CHUNKS, 2)),
            dma((CHUNKS + 1, chips)),
            dma((CHUNKS + 1, chips)),
        ],
        compiler_params=pltpu.CompilerParams(
            collective_id=0, has_side_effects=True, vmem_limit_bytes=60 * 1024 * 1024
        ),
    )(queries, question_keys, question_values, doc_keys, doc_values, lengths, offsets)


def solution(mesh):
    placed = (
        P(("grp", "seq"), None),
        P(("grp", "seq"), None),
        P(("grp", "seq"), None),
        P(("grp", "seq"), None),
        P(("grp", "seq"), None),
        P("grp"),
        P("grp"),
    )
    return jax.shard_map(
        functools.partial(fused, mesh.shape["seq"]),
        mesh=mesh, in_specs=placed, out_specs=P(("grp", "seq"), None), check_vma=False,
    )
```
